32 devices in a mesh: gx: 4 (over x, core), gy: 8 (over z, y).
Axes of the slice: x: 2, y: 2, z: 4, core: 2. Of those that a mesh axis runs over, the one named last changes fastest.
Arguments:
- substrate: float32 [16, 64, 1024], P(None, 'gy', 'gx'), may hold values from 0 to 1
- catalyst: float32 [16, 64, 1024], P(None, 'gy', 'gx'), may hold values from 0 to 1
Outputs:
- substrate_next: float32 [16, 64, 1024], P(None, 'gy', 'gx')
- catalyst_next: float32 [16, 64, 1024], P(None, 'gy', 'gx')
- rebuilt: float32 [2, 16, 1024, 64], P(None, None, ('gx', 'gy'))
The draws below stay inside these ranges and needn't reach their ends.
All inputs are finite; a program needn't handle non-finite values.
Results may differ from the reference program's by a relative error of at most 0.00002.
Values sent between devices are 32-bit elements; how exact they have to be, the bound alone decides.
A program may use at most 64 MiB of HBM per device.

```python
import jax
import jax.numpy as jnp

Z = 16
NX = 1024
NY = 64


def block_scale(rng, extent, split, low, largest):
    def one(axis_at, shards_of):
        heights = jax.random.uniform(jax.random.fold_in(jax.random.fold_in(rng, 6), axis_at), (shards_of,), jnp.float32, low / len(split), largest / len(split))
        return jnp.repeat(jnp.exp(heights), extent[axis_at] // shards_of).reshape((-1,) + (1,) * (len(extent) - axis_at - 1))

    gain = one(*split[0])
    for cut in split[1:]:
        gain = gain * one(*cut)
    return gain


def setup_inputs(seed: int = 0) -> dict:
    seeds = jax.random.split(jax.random.key(seed), 3)
    return {
        "substrate": jnp.clip(1.0 * jax.random.uniform(seeds[0], (Z, NY, NX), jnp.float32) ** block_scale(seeds[0], (Z, NY, NX), ((1, 8), (2, 4)), -0.2, 0.2), 0.0, 1.0),
        "catalyst": jnp.clip(1.0 * jax.random.uniform(seeds[1], (Z, NY, NX), jnp.float32) ** block_scale(seeds[1], (Z, NY, NX), ((1, 8), (2, 4)), -0.2, 0.2), 0.0, 1.0),
    }


feed_rate = 0.037
kill_rate = 0.06
substrate_diffusion = 0.15
catalyst_diffusion = 0.08


def react(center, spread):
    substrate = center[0]
    catalyst = center[1]
    reaction = substrate * catalyst * catalyst
    new_substrate = substrate + substrate_diffusion * spread[0] - reaction + feed_rate * (1.0 - substrate)
    new_catalyst = catalyst + catalyst_diffusion * spread[1] + reaction - (feed_rate + kill_rate) * catalyst
    return jnp.stack([new_substrate, new_catalyst])


def neighbours(field):
    total = jnp.roll(field, 1, 1) + jnp.roll(field, -1, 1)
    total = total + jnp.roll(field, 1, 2) + jnp.roll(field, -1, 2)
    total = total + jnp.roll(field, 1, 3) + jnp.roll(field, -1, 3)
    return total - 6.0 * field


def restrict(field):
    shape = field.shape
    blocks = field.reshape(shape[0], shape[1], shape[2] // 2, 2, shape[3] // 2, 2)
    return (blocks[:, :, :, 0, :, 0] + blocks[:, :, :, 0, :, 1] + blocks[:, :, :, 1, :, 0] + blocks[:, :, :, 1, :, 1]) * 0.25


def prolong(field):
    return jnp.repeat(jnp.repeat(field, 2, axis=2), 2, axis=3)


def reference(substrate, catalyst):
    state = jnp.stack([substrate, catalyst])
    state = react(state, neighbours(state))
    state = react(state, neighbours(state))
    level1 = restrict(state)
    level2 = restrict(level1)
    coarse = prolong(level2)
    blend = coarse + 0.5 * (level1 - coarse)
    rebuilt = jnp.swapaxes(prolong(blend), 2, 3)
    return state[0], state[1], rebuilt
```

```python
import functools

import jax
import jax.numpy as jnp
from jax import lax
from jax.experimental import pallas as pl
from jax.experimental.pallas import tpu as pltpu
from jax.sharding import PartitionSpec as P

feed_rate = 0.037
kill_rate = 0.06
substrate_diffusion = 0.15
catalyst_diffusion = 0.08

MESH = pl.DeviceIdType.MESH
LANES = 128


def react(substrate, catalyst, spread_substrate, spread_catalyst):
    reaction = substrate * catalyst * catalyst
    new_substrate = (
        substrate
        + substrate_diffusion * spread_substrate
        - reaction
        + feed_rate * (1.0 - substrate)
    )
    new_catalyst = (
        catalyst
        + catalyst_diffusion * spread_catalyst
        + reaction
        - (feed_rate + kill_rate) * catalyst
    )
    return new_substrate, new_catalyst


def split(value):
    high = value.astype(jnp.bfloat16)
    low = (value - high.astype(jnp.float32)).astype(jnp.bfloat16)
    return high, low


def spread_of(before, here, after):
    planes, extent = here.shape
    total = pltpu.roll(here, 1, 0) + pltpu.roll(here, planes - 1, 0)
    total = total + before + after
    total = total + pltpu.roll(here, 1, 1) + pltpu.roll(here, extent - 1, 1)
    return total - 6.0 * here


def kernel(dims, fused, *refs):
    planes, columns, extent, owners, slabs_x, slabs_y = dims
    (u_ref, v_ref, u_out, v_out, last_out, loaded, state, edge, packed, got, middle, sums,
     outgoing, incoming, doubled, load_sem, send_sem, recv_sem, deal_send, deal_recv) = refs
    gathered = incoming if fused else last_out
    tiles = extent // LANES
    gx, gy = lax.axis_index("gx"), lax.axis_index("gy")

    barrier = pltpu.get_barrier_semaphore()
    sides = [
        (lax.rem(gx + slabs_x + dx, slabs_x), lax.rem(gy + slabs_y + dy, slabs_y))
        for dx in (-1, 1)
        for dy in (-1, 0, 1)
    ]
    peers = [(gx, lax.rem(gy + step, owners)) for step in range(1, owners)]
    for device in sides + peers:
        pl.semaphore_signal(barrier, inc=1, device_id=device, device_id_type=MESH)

    loads = [
        pltpu.make_async_copy(source, loaded.at[field], load_sem.at[field])
        for field, source in enumerate((u_ref, v_ref))
    ]
    for load in loads:
        load.start()
    for load in loads:
        load.wait()

    lane = lax.broadcasted_iota(jnp.int32, (planes, LANES), 1)
    group = lax.rem(lane + 2, LANES) // 4
    pack = jnp.zeros((planes, LANES), jnp.float32)
    for field in range(2):
        for column in range(columns):
            slab = jnp.concatenate(
                [
                    loaded[field, pl.ds(tile * columns + column, planes, stride=tiles * columns), :]
                    for tile in range(tiles)
                ],
                axis=1,
            )
            state[field, 2 + column] = slab
            at = field * columns + column
            ends = jnp.where(lane < LANES // 2, slab[:, :LANES], slab[:, extent - LANES :])
            ends = pltpu.roll(ends, 4 * at, 1) if at else ends
            pack = jnp.where(group == at, ends, pack)
    packed[...] = pack

    pl.semaphore_wait(barrier, len(sides) + len(peers))

    copies = []
    for side, (target, source) in enumerate(((slice(0, 2), slice(columns, columns + 2)),
                                             (slice(columns + 2, columns + 4), slice(2, 4)))):
        there = lax.rem(gy + (1 if side == 0 else slabs_y - 1), slabs_y)
        copies.append(
            pltpu.make_async_remote_copy(
                src_ref=state.at[:, source],
                dst_ref=state.at[:, target],
                send_sem=send_sem.at[side],
                recv_sem=recv_sem.at[side],
                device_id=(gx, there),
                device_id_type=MESH,
            )
        )
    for number, device in enumerate(sides):
        a, b = (1 - number // 3, 2 - number % 3)
        copies.append(
            pltpu.make_async_remote_copy(
                src_ref=packed,
                dst_ref=got.at[a, b],
                send_sem=send_sem.at[2 + number],
                recv_sem=recv_sem.at[2 + 3 * a + b],
                device_id=device,
                device_id_type=MESH,
            )
        )
    for copy in copies:
        copy.start()

    half = extent // 2
    row = lax.broadcasted_iota(jnp.int32, (half, extent), 0)
    fine = lax.broadcasted_iota(jnp.int32, (half, extent), 1)
    to_blend = jnp.concatenate(
        [
            jnp.where(fine // 2 == row, 0.125, 0.0),
            jnp.where(fine // 4 == row // 2, 0.03125, 0.0),
        ],
        axis=1,
    ).astype(jnp.bfloat16)

    for side in range(2):
        for b in range(3):
            slot = 2 + 3 * side + b
            pltpu.make_async_remote_copy(
                src_ref=packed,
                dst_ref=got.at[side, b],
                send_sem=send_sem.at[slot],
                recv_sem=recv_sem.at[slot],
                device_id=sides[3 * (1 - side) + 2 - b],
                device_id_type=MESH,
            ).wait_recv()
    for side in range(2):
        copies[side].wait_recv()

    both = [jnp.where(lax.rem(lane, 4) < 2, got[1, b], got[0, b]) for b in range(3)]
    for field in range(2):
        for c in range(1, columns + 3):
            if c == 1:
                b, at = 0, field * columns + columns - 1
            elif c == columns + 2:
                b, at = 2, field * columns
            else:
                b, at = 1, field * columns + c - 2
            edge[field, c] = pltpu.roll(both[b], LANES - 4 * at, 1) if at else both[b]

    def wide(field, c):
        if c in (0, columns + 3):
            tail = jnp.zeros((planes, LANES), jnp.float32)
        else:
            tail = edge[field, c]
        return jnp.concatenate([state[field, c], tail], axis=1)

    for c in range(1, columns + 3):
        u, v = wide(0, c), wide(1, c)
        su = spread_of(wide(0, c - 1), u, wide(0, c + 1))
        sv = spread_of(wide(1, c - 1), v, wide(1, c + 1))
        middle[0, c], middle[1, c] = react(u, v, su, sv)

    level = [[], []]
    for c in range(2, columns + 2):
        u, v = middle[0, c], middle[1, c]
        su = spread_of(middle[0, c - 1], u, middle[0, c + 1])
        sv = spread_of(middle[1, c - 1], v, middle[1, c + 1])
        new = react(u[:, :extent], v[:, :extent], su[:, :extent], sv[:, :extent])
        for field, out in enumerate((u_out, v_out)):
            for tile in range(tiles):
                rows = pl.ds(tile * columns + c - 2, planes, stride=tiles * columns)
                out[rows, :] = new[field][:, tile * LANES : (tile + 1) * LANES]
            level[field].append(new[field])

    pairs = columns // 2
    for field in range(2):
        twos = [level[field][2 * k] + level[field][2 * k + 1] for k in range(pairs)]
        fours = [twos[2 * q] + twos[2 * q + 1] for q in range(pairs // 2)]
        for k in range(pairs):
            rows = pl.ds(field * planes * pairs + k, planes, stride=pairs)
            for tile in range(tiles):
                lanes = slice(tile * LANES, (tile + 1) * LANES)
                sums[tile, rows, :] = twos[k][:, lanes]
                sums[tiles + tile, rows, :] = fours[k // 2][:, lanes]

    contract = (((1,), (1,)), ((), ()))
    high, low = split(jnp.concatenate([sums[tile] for tile in range(2 * tiles)], axis=1))
    blend = lax.dot_general(to_blend, high, contract, preferred_element_type=jnp.float32)
    blend += lax.dot_general(to_blend, low, contract, preferred_element_type=jnp.float32)
    portion = half // owners
    for owner in range(owners):
        outgoing[owner] = blend[owner * portion : (owner + 1) * portion]

    deals = []
    for step in range(1, owners):
        deals.append(
            pltpu.make_async_remote_copy(
                src_ref=outgoing.at[lax.rem(gy + step, owners)],
                dst_ref=gathered.at[gy],
                send_sem=deal_send.at[step - 1],
                recv_sem=deal_recv.at[step - 1],
                device_id=(gx, lax.rem(gy + step, owners)),
                device_id_type=MESH,
            )
        )
        deals[-1].start()
    gathered[gy] = outgoing[gy]

    if fused:
        wide_in = lax.broadcasted_iota(jnp.int32, (LANES, 4 * LANES), 0)
        wide_out = lax.broadcasted_iota(jnp.int32, (LANES, 4 * LANES), 1)
        column_of = wide_in // 16 * 4 + wide_in % 4
        spreading = jnp.where(
            (wide_in // 4 % 4 == wide_out // LANES) & (column_of == wide_out % LANES // 2),
            1.0,
            0.0,
        ).astype(jnp.bfloat16)
        lane = lax.broadcasted_iota(jnp.int32, (portion, LANES), 1)

    for deal in deals:
        deal.wait_recv()

    if fused:
        blocks = [incoming[owner] for owner in range(owners)]
        for h in range(8):
            part = jnp.zeros((portion, LANES), jnp.float32)
            for owner in range(8):
                shift = (16 * (owner - h)) % LANES
                moved = pltpu.roll(blocks[owner], shift, 1) if shift else blocks[owner]
                part = jnp.where(lane // 16 == owner, moved, part)
            doubled[pl.ds(2 * h * portion, portion, stride=2), :] = part
            doubled[pl.ds(2 * h * portion + 1, portion, stride=2), :] = part
        high, low = split(doubled[...])
        whole = jnp.dot(high, spreading, preferred_element_type=jnp.float32)
        whole += jnp.dot(low, spreading, preferred_element_type=jnp.float32)
        width, rows = last_out.shape[1], 2 * portion
        for h in range(8):
            for z in range(4):
                base = (h * 4 + z) * rows
                last_out[base : base + rows, :] = whole[
                    h * rows : (h + 1) * rows, z * LANES : z * LANES + width
                ]

    for copy in copies:
        copy.wait_send()
    for deal in deals:
        deal.wait_send()


def tiled(field):
    planes, columns, extent = field.shape
    field = field.reshape(planes, columns, extent // LANES, LANES)
    return jnp.transpose(field, (0, 2, 1, 3)).reshape(-1, LANES)


def untiled(field, shape):
    planes, columns, extent = shape
    field = field.reshape(planes, extent // LANES, columns, LANES)
    return jnp.transpose(field, (0, 2, 1, 3)).reshape(shape)


def body(substrate, catalyst):
    planes, columns, extent = substrate.shape
    slabs_x, owners = lax.axis_size("gx"), lax.axis_size("gy")
    half, pairs, tiles = extent // 2, columns // 2, extent // LANES
    portion = half // owners
    values = 2 * planes * pairs
    fused = (
        planes == 16 and pairs == 4 and owners == 8 and values == LANES and portion % 8 == 0
    )
    dims = (planes, columns, extent, owners, slabs_x, owners)
    flat = jax.ShapeDtypeStruct((planes * tiles * columns, LANES), jnp.float32)
    dealt = jax.ShapeDtypeStruct((owners, portion, values), jnp.float32)
    rebuilt_rows = 2 * portion
    last = (
        jax.ShapeDtypeStruct((2 * planes * rebuilt_rows, columns * owners), jnp.float32)
        if fused
        else dealt
    )
    vmem = pl.BlockSpec(memory_space=pltpu.VMEM)
    f32 = jnp.float32
    u, v, final = pl.pallas_call(
        functools.partial(kernel, dims, fused),
        out_shape=(flat, flat, last),
        in_specs=[pl.BlockSpec(memory_space=pl.ANY)] * 2,
        out_specs=(vmem, vmem, vmem),
        scratch_shapes=[
            pltpu.VMEM((2, planes * tiles * columns, LANES), f32),
            pltpu.VMEM((2, columns + 4, planes, extent), f32),
            pltpu.VMEM((2, columns + 4, planes, LANES), f32),
            pltpu.VMEM((planes, LANES), f32),
            pltpu.VMEM((2, 3, planes, LANES), f32),
            pltpu.VMEM((2, columns + 4, planes, extent + LANES), f32),
            pltpu.VMEM((2 * tiles, values, LANES), f32),
            pltpu.VMEM((owners, portion, values), f32),
            pltpu.VMEM((owners, portion, values) if fused else (8, LANES), f32),
            pltpu.VMEM((16 * portion, LANES), f32),
            pltpu.SemaphoreType.DMA((2,)),
            pltpu.SemaphoreType.DMA((8,)),
            pltpu.SemaphoreType.DMA((8,)),
            pltpu.SemaphoreType.DMA((owners - 1,)),
            pltpu.SemaphoreType.DMA((owners - 1,)),
        ],
        compiler_params=pltpu.CompilerParams(collective_id=0, has_side_effects=True),
    )(
        tiled(substrate),
        tiled(catalyst),
    )
    if fused:
        rebuilt = final.reshape(2, planes, rebuilt_rows, columns * owners)
    else:
        blend = final.reshape(owners, portion, 2, planes, pairs)
        blend = jnp.transpose(blend, (2, 3, 1, 0, 4)).reshape(2, planes, portion, owners * pairs)
        rebuilt = jnp.repeat(jnp.repeat(blend, 2, axis=2), 2, axis=3)
    return untiled(u, substrate.shape), untiled(v, substrate.shape), rebuilt


def solution(mesh):
    in_specs = (P(None, "gy", "gx"), P(None, "gy", "gx"))
    out_specs = (P(None, "gy", "gx"), P(None, "gy", "gx"), P(None, None, ("gx", "gy"), None))
    return jax.shard_map(body, mesh=mesh, in_specs=in_specs, out_specs=out_specs, check_vma=False)
```

```python
import functools

import jax
import jax.numpy as jnp
from jax import lax
from jax.experimental import pallas as pl
from jax.experimental.pallas import tpu as pltpu
from jax.sharding import PartitionSpec as P

feed_rate = 0.037
kill_rate = 0.06
substrate_diffusion = 0.15
catalyst_diffusion = 0.08

MESH = pl.DeviceIdType.MESH
LANES = 128


def react(substrate, catalyst, spread_substrate, spread_catalyst):
    reaction = substrate * catalyst * catalyst
    new_substrate = (
        substrate
        + substrate_diffusion * spread_substrate
        - reaction
        + feed_rate * (1.0 - substrate)
    )
    new_catalyst = (
        catalyst
        + catalyst_diffusion * spread_catalyst
        + reaction
        - (feed_rate + kill_rate) * catalyst
    )
    return new_substrate, new_catalyst


def split(value):
    high = value.astype(jnp.bfloat16)
    low = (value - high.astype(jnp.float32)).astype(jnp.bfloat16)
    return high, low


def spread_of(before, here, after):
    planes, extent = here.shape
    total = pltpu.roll(here, 1, 0) + pltpu.roll(here, planes - 1, 0)
    total = total + before + after
    total = total + pltpu.roll(here, 1, 1) + pltpu.roll(here, extent - 1, 1)
    return total - 6.0 * here


def kernel(dims, *refs):
    planes, columns, extent, owners, slabs_x, slabs_y = dims
    (u_ref, v_ref, u_out, v_out, gathered, loaded, state, edge, packed, got, middle, sums,
     outgoing, load_sem, send_sem, recv_sem, deal_send, deal_recv) = refs
    tiles = extent // LANES
    gx, gy = lax.axis_index("gx"), lax.axis_index("gy")

    barrier = pltpu.get_barrier_semaphore()
    sides = [
        (lax.rem(gx + slabs_x + dx, slabs_x), lax.rem(gy + slabs_y + dy, slabs_y))
        for dx in (-1, 1)
        for dy in (-1, 0, 1)
    ]
    peers = [(gx, lax.rem(gy + step, owners)) for step in range(1, owners)]
    for device in sides + peers:
        pl.semaphore_signal(barrier, inc=1, device_id=device, device_id_type=MESH)

    loads = [
        pltpu.make_async_copy(source, loaded.at[field], load_sem.at[field])
        for field, source in enumerate((u_ref, v_ref))
    ]
    for load in loads:
        load.start()
    for load in loads:
        load.wait()

    lane = lax.broadcasted_iota(jnp.int32, (planes, LANES), 1)
    group = lax.rem(lane + 2, LANES) // 4
    pack = jnp.zeros((planes, LANES), jnp.float32)
    for field in range(2):
        for column in range(columns):
            slab = jnp.concatenate(
                [
                    loaded[field, pl.ds(tile * columns + column, planes, stride=tiles * columns), :]
                    for tile in range(tiles)
                ],
                axis=1,
            )
            state[field, 2 + column] = slab
            at = field * columns + column
            ends = jnp.where(lane < LANES // 2, slab[:, :LANES], slab[:, extent - LANES :])
            ends = pltpu.roll(ends, 4 * at, 1) if at else ends
            pack = jnp.where(group == at, ends, pack)
    packed[...] = pack

    pl.semaphore_wait(barrier, len(sides) + len(peers))

    copies = []
    for side, (target, source) in enumerate(((slice(0, 2), slice(columns, columns + 2)),
                                             (slice(columns + 2, columns + 4), slice(2, 4)))):
        there = lax.rem(gy + (1 if side == 0 else slabs_y - 1), slabs_y)
        copies.append(
            pltpu.make_async_remote_copy(
                src_ref=state.at[:, source],
                dst_ref=state.at[:, target],
                send_sem=send_sem.at[side],
                recv_sem=recv_sem.at[side],
                device_id=(gx, there),
                device_id_type=MESH,
            )
        )
    for number, device in enumerate(sides):
        a, b = (1 - number // 3, 2 - number % 3)
        copies.append(
            pltpu.make_async_remote_copy(
                src_ref=packed,
                dst_ref=got.at[a, b],
                send_sem=send_sem.at[2 + number],
                recv_sem=recv_sem.at[2 + 3 * a + b],
                device_id=device,
                device_id_type=MESH,
            )
        )
    for copy in copies:
        copy.start()

    half = extent // 2
    row = lax.broadcasted_iota(jnp.int32, (half, extent), 0)
    fine = lax.broadcasted_iota(jnp.int32, (half, extent), 1)
    to_blend = jnp.concatenate(
        [
            jnp.where(fine // 2 == row, 0.125, 0.0),
            jnp.where(fine // 4 == row // 2, 0.03125, 0.0),
        ],
        axis=1,
    ).astype(jnp.bfloat16)

    for side in range(2):
        for b in range(3):
            slot = 2 + 3 * side + b
            pltpu.make_async_remote_copy(
                src_ref=packed,
                dst_ref=got.at[side, b],
                send_sem=send_sem.at[slot],
                recv_sem=recv_sem.at[slot],
                device_id=sides[3 * (1 - side) + 2 - b],
                device_id_type=MESH,
            ).wait_recv()
    for side in range(2):
        copies[side].wait_recv()

    both = [jnp.where(lax.rem(lane, 4) < 2, got[1, b], got[0, b]) for b in range(3)]
    for field in range(2):
        for c in range(1, columns + 3):
            if c == 1:
                b, at = 0, field * columns + columns - 1
            elif c == columns + 2:
                b, at = 2, field * columns
            else:
                b, at = 1, field * columns + c - 2
            edge[field, c] = pltpu.roll(both[b], LANES - 4 * at, 1) if at else both[b]

    def wide(field, c):
        if c in (0, columns + 3):
            tail = jnp.zeros((planes, LANES), jnp.float32)
        else:
            tail = edge[field, c]
        return jnp.concatenate([state[field, c], tail], axis=1)

    for c in range(1, columns + 3):
        u, v = wide(0, c), wide(1, c)
        su = spread_of(wide(0, c - 1), u, wide(0, c + 1))
        sv = spread_of(wide(1, c - 1), v, wide(1, c + 1))
        middle[0, c], middle[1, c] = react(u, v, su, sv)

    level = [[], []]
    for c in range(2, columns + 2):
        u, v = middle[0, c], middle[1, c]
        su = spread_of(middle[0, c - 1], u, middle[0, c + 1])
        sv = spread_of(middle[1, c - 1], v, middle[1, c + 1])
        new = react(u[:, :extent], v[:, :extent], su[:, :extent], sv[:, :extent])
        for field, out in enumerate((u_out, v_out)):
            for tile in range(tiles):
                rows = pl.ds(tile * columns + c - 2, planes, stride=tiles * columns)
                out[rows, :] = new[field][:, tile * LANES : (tile + 1) * LANES]
            level[field].append(new[field])

    pairs = columns // 2
    for field in range(2):
        twos = [level[field][2 * k] + level[field][2 * k + 1] for k in range(pairs)]
        fours = [twos[2 * q] + twos[2 * q + 1] for q in range(pairs // 2)]
        for k in range(pairs):
            rows = pl.ds(field * planes * pairs + k, planes, stride=pairs)
            for tile in range(tiles):
                lanes = slice(tile * LANES, (tile + 1) * LANES)
                sums[tile, rows, :] = twos[k][:, lanes]
                sums[tiles + tile, rows, :] = fours[k // 2][:, lanes]

    contract = (((1,), (1,)), ((), ()))
    high, low = split(jnp.concatenate([sums[tile] for tile in range(2 * tiles)], axis=1))
    blend = lax.dot_general(to_blend, high, contract, preferred_element_type=jnp.float32)
    blend += lax.dot_general(to_blend, low, contract, preferred_element_type=jnp.float32)
    portion = half // owners
    for owner in range(owners):
        outgoing[owner] = blend[owner * portion : (owner + 1) * portion]

    deals = []
    for step in range(1, owners):
        deals.append(
            pltpu.make_async_remote_copy(
                src_ref=outgoing.at[lax.rem(gy + step, owners)],
                dst_ref=gathered.at[gy],
                send_sem=deal_send.at[step - 1],
                recv_sem=deal_recv.at[step - 1],
                device_id=(gx, lax.rem(gy + step, owners)),
                device_id_type=MESH,
            )
        )
        deals[-1].start()
    gathered[gy] = outgoing[gy]

    for deal in deals:
        deal.wait_recv()

    for copy in copies:
        copy.wait_send()
    for deal in deals:
        deal.wait_send()


def finish(u_ref, v_ref, dealt, u_out, v_out, rebuilt_out, doubled, rebuilt, sems):
    copies = [
        pltpu.make_async_copy(u_ref, u_out, sems.at[0]),
        pltpu.make_async_copy(v_ref, v_out, sems.at[1]),
    ]
    for copy in copies:
        copy.start()

    owners, portion, _ = dealt.shape
    wide_in = lax.broadcasted_iota(jnp.int32, (LANES, 4 * LANES), 0)
    wide_out = lax.broadcasted_iota(jnp.int32, (LANES, 4 * LANES), 1)
    column_of = wide_in // 16 * 4 + wide_in % 4
    spreading = jnp.where(
        (wide_in // 4 % 4 == wide_out // LANES) & (column_of == wide_out % LANES // 2),
        1.0,
        0.0,
    ).astype(jnp.bfloat16)
    lane = lax.broadcasted_iota(jnp.int32, (portion, LANES), 1)
    blocks = [dealt[owner] for owner in range(owners)]
    width, rows = rebuilt.shape[1], 2 * portion
    chunks = 4
    share = 8 // chunks
    for chunk in range(chunks):
        for h in range(chunk * share, (chunk + 1) * share):
            part = jnp.zeros((portion, LANES), jnp.float32)
            for owner in range(8):
                shift = (16 * (owner - h)) % LANES
                moved = pltpu.roll(blocks[owner], shift, 1) if shift else blocks[owner]
                part = jnp.where(lane // 16 == owner, moved, part)
            doubled[pl.ds(h * rows, portion, stride=2), :] = part
            doubled[pl.ds(h * rows + 1, portion, stride=2), :] = part
        high, low = split(doubled[chunk * share * rows : (chunk + 1) * share * rows, :])
        whole = jnp.dot(high, spreading, preferred_element_type=jnp.float32)
        whole += jnp.dot(low, spreading, preferred_element_type=jnp.float32)
        for h in range(share):
            for z in range(4):
                base = ((chunk * share + h) * 4 + z) * rows
                rebuilt[base : base + rows, :] = whole[
                    h * rows : (h + 1) * rows, z * LANES : z * LANES + width
                ]
        size = share * 4 * rows
        copies.append(
            pltpu.make_async_copy(
                rebuilt.at[chunk * size : (chunk + 1) * size],
                rebuilt_out.at[chunk * size : (chunk + 1) * size],
                sems.at[2 + chunk],
            )
        )
        copies[-1].start()
    for copy in copies:
        copy.wait()


def tiled(field):
    planes, columns, extent = field.shape
    field = field.reshape(planes, columns, extent // LANES, LANES)
    return jnp.transpose(field, (0, 2, 1, 3)).reshape(-1, LANES)


def untiled(field, shape):
    planes, columns, extent = shape
    field = field.reshape(planes, extent // LANES, columns, LANES)
    return jnp.transpose(field, (0, 2, 1, 3)).reshape(shape)


def body(substrate, catalyst):
    planes, columns, extent = substrate.shape
    slabs_x, owners = lax.axis_size("gx"), lax.axis_size("gy")
    half, pairs, tiles = extent // 2, columns // 2, extent // LANES
    portion = half // owners
    values = 2 * planes * pairs
    fused = (
        planes == 16 and pairs == 4 and owners == 8 and values == LANES and portion % 8 == 0
    )
    dims = (planes, columns, extent, owners, slabs_x, owners)
    f32 = jnp.float32
    flat = (planes * tiles * columns, LANES)
    vmem = pl.BlockSpec(memory_space=pltpu.VMEM)
    anywhere = pl.BlockSpec(memory_space=pl.ANY)
    u, v, dealt = pl.pallas_call(
        functools.partial(kernel, dims),
        out_shape=(
            pltpu.VMEM(flat, f32),
            pltpu.VMEM(flat, f32),
            pltpu.VMEM((owners, portion, values), f32),
        ),
        in_specs=[anywhere] * 2,
        out_specs=(vmem,) * 3,
        scratch_shapes=[
            pltpu.VMEM((2,) + flat, f32),
            pltpu.VMEM((2, columns + 4, planes, extent), f32),
            pltpu.VMEM((2, columns + 4, planes, LANES), f32),
            pltpu.VMEM((planes, LANES), f32),
            pltpu.VMEM((2, 3, planes, LANES), f32),
            pltpu.VMEM((2, columns + 4, planes, extent + LANES), f32),
            pltpu.VMEM((2 * tiles, values, LANES), f32),
            pltpu.VMEM((owners, portion, values), f32),
            pltpu.SemaphoreType.DMA((2,)),
            pltpu.SemaphoreType.DMA((8,)),
            pltpu.SemaphoreType.DMA((8,)),
            pltpu.SemaphoreType.DMA((owners - 1,)),
            pltpu.SemaphoreType.DMA((owners - 1,)),
        ],
        compiler_params=pltpu.CompilerParams(collective_id=0, has_side_effects=True),
    )(tiled(substrate), tiled(catalyst))
    rows, width = 2 * portion, columns * owners
    if fused:
        u, v, dealt = (
            pltpu.with_memory_space_constraint(x, pltpu.VMEM) for x in (u, v, dealt)
        )
        u, v, rebuilt = pl.pallas_call(
            finish,
            out_shape=(
                jax.ShapeDtypeStruct(flat, f32),
                jax.ShapeDtypeStruct(flat, f32),
                jax.ShapeDtypeStruct((2 * planes * rows, width), f32),
            ),
            in_specs=[vmem] * 3,
            out_specs=(anywhere,) * 3,
            scratch_shapes=[
                pltpu.VMEM((8 * rows, LANES), f32),
                pltpu.VMEM((2 * planes * rows, width), f32),
                pltpu.SemaphoreType.DMA((6,)),
            ],
        )(u, v, dealt)
        rebuilt = rebuilt.reshape(2, planes, rows, width)
    else:
        blend = dealt.reshape(owners, portion, 2, planes, pairs)
        blend = jnp.transpose(blend, (2, 3, 1, 0, 4)).reshape(2, planes, portion, owners * pairs)
        rebuilt = jnp.repeat(jnp.repeat(blend, 2, axis=2), 2, axis=3)
    return untiled(u, substrate.shape), untiled(v, substrate.shape), rebuilt


def solution(mesh):
    in_specs = (P(None, "gy", "gx"), P(None, "gy", "gx"))
    out_specs = (P(None, "gy", "gx"), P(None, "gy", "gx"), P(None, None, ("gx", "gy"), None))
    return jax.shard_map(body, mesh=mesh, in_specs=in_specs, out_specs=out_specs, check_vma=False)
```

```python
import functools

import jax
import jax.numpy as jnp
from jax import lax
from jax.experimental import pallas as pl
from jax.experimental.pallas import tpu as pltpu
from jax.sharding import PartitionSpec as P

feed_rate = 0.037
kill_rate = 0.06
substrate_diffusion = 0.15
catalyst_diffusion = 0.08

MESH = pl.DeviceIdType.MESH
LANES = 128


def react(substrate, catalyst, spread_substrate, spread_catalyst):
    reaction = substrate * catalyst * catalyst
    new_substrate = (
        substrate
        + substrate_diffusion * spread_substrate
        - reaction
        + feed_rate * (1.0 - substrate)
    )
    new_catalyst = (
        catalyst
        + catalyst_diffusion * spread_catalyst
        + reaction
        - (feed_rate + kill_rate) * catalyst
    )
    return new_substrate, new_catalyst


def split(value):
    high = value.astype(jnp.bfloat16)
    low = (value - high.astype(jnp.float32)).astype(jnp.bfloat16)
    return high, low


def spread_of(before, here, after):
    planes, extent = here.shape
    total = pltpu.roll(here, 1, 0) + pltpu.roll(here, planes - 1, 0)
    total = total + before + after
    total = total + pltpu.roll(here, 1, 1) + pltpu.roll(here, extent - 1, 1)
    return total - 6.0 * here


def partner_of(me, step, size):
    if size & (size - 1):
        return lax.rem(me + step, size)
    partner = me + step
    for bit in range(size.bit_length() - 1):
        if step >> bit & 1:
            partner = partner - 2 * (1 << bit) * lax.rem(me // (1 << bit), 2)
    return partner


def kernel(dims, *refs):
    planes, columns, extent, owners, slabs_x, slabs_y = dims
    (u_ref, v_ref, u_out, v_out, gathered, loaded, state, edge, packed, got, relay, relayed, middle, sums,
     outgoing, load_sem, send_sem, recv_sem, deal_send, deal_recv) = refs
    tiles = extent // LANES
    gx, gy = lax.axis_index("gx"), lax.axis_index("gy")

    barrier = pltpu.get_barrier_semaphore()
    sides = [(lax.rem(gx + shift, slabs_x), gy) for shift in (1, slabs_x - 1)]
    ends = [(gx, lax.rem(gy + shift, owners)) for shift in (1, owners - 1)]
    peers = [(gx, lax.rem(gy + step, owners)) for step in range(1, owners)]
    for device in sides + peers:
        pl.semaphore_signal(barrier, inc=1, device_id=device, device_id_type=MESH)

    loads = [
        pltpu.make_async_copy(source, loaded.at[field], load_sem.at[field])
        for field, source in enumerate((u_ref, v_ref))
    ]
    for load in loads:
        load.start()
    for load in loads:
        load.wait()

    lane = lax.broadcasted_iota(jnp.int32, (planes, LANES), 1)
    group = lax.rem(lane + 2, LANES) // 4
    pack = jnp.zeros((planes, LANES), jnp.float32)
    for field in range(2):
        for column in range(columns):
            slab = jnp.concatenate(
                [
                    loaded[field, pl.ds(tile * columns + column, planes, stride=tiles * columns), :]
                    for tile in range(tiles)
                ],
                axis=1,
            )
            state[field, 2 + column] = slab
            at = field * columns + column
            tips = jnp.where(lane < LANES // 2, slab[:, :LANES], slab[:, extent - LANES :])
            tips = pltpu.roll(tips, 4 * at, 1) if at else tips
            pack = jnp.where(group == at, tips, pack)
    packed[...] = pack

    pl.semaphore_wait(barrier, len(sides) + len(peers))

    def send(number, source, target, device):
        return pltpu.make_async_remote_copy(
            src_ref=source,
            dst_ref=target,
            send_sem=send_sem.at[number],
            recv_sem=recv_sem.at[number],
            device_id=device,
            device_id_type=MESH,
        )

    low_end, high_end = slice(0, 2), slice(columns + 2, columns + 4)
    across = [send(2 + side, packed, got.at[side], sides[side]) for side in range(2)]
    along = [
        send(0, state.at[:, columns : columns + 2], state.at[:, low_end], ends[0]),
        send(1, state.at[:, 2:4], state.at[:, high_end], ends[1]),
    ]
    corners = [send(4 + side, relay, relayed.at[side], ends[side]) for side in range(2)]
    for copy in across + along:
        copy.start()

    half = extent // 2
    row = lax.broadcasted_iota(jnp.int32, (half, extent), 0)
    fine = lax.broadcasted_iota(jnp.int32, (half, extent), 1)
    to_blend = jnp.concatenate(
        [
            jnp.where(fine // 2 == row, 0.125, 0.0),
            jnp.where(fine // 4 == row // 2, 0.03125, 0.0),
        ],
        axis=1,
    ).astype(jnp.bfloat16)

    for copy in across:
        copy.wait_recv()

    both = jnp.where(lax.rem(lane, 4) < 2, got[1], got[0])
    relay[...] = both

    def place(field, c, tile, column):
        at = field * columns + column
        edge[field, c] = pltpu.roll(tile, LANES - 4 * at, 1) if at else tile

    for field in range(2):
        for c in range(2, columns + 2):
            place(field, c, both, c - 2)
    for copy in corners:
        copy.start()

    def wide(field, c):
        if c in (0, columns + 3):
            tail = jnp.zeros((planes, LANES), jnp.float32)
        else:
            tail = edge[field, c]
        return jnp.concatenate([state[field, c], tail], axis=1)

    def first(c):
        u, v = wide(0, c), wide(1, c)
        su = spread_of(wide(0, c - 1), u, wide(0, c + 1))
        sv = spread_of(wide(1, c - 1), v, wide(1, c + 1))
        middle[0, c], middle[1, c] = react(u, v, su, sv)

    level = [{}, {}]

    def second(c):
        u, v = middle[0, c], middle[1, c]
        su = spread_of(middle[0, c - 1], u, middle[0, c + 1])
        sv = spread_of(middle[1, c - 1], v, middle[1, c + 1])
        new = react(u[:, :extent], v[:, :extent], su[:, :extent], sv[:, :extent])
        for field, out in enumerate((u_out, v_out)):
            for tile in range(tiles):
                rows = pl.ds(tile * columns + c - 2, planes, stride=tiles * columns)
                out[rows, :] = new[field][:, tile * LANES : (tile + 1) * LANES]
            level[field][c - 2] = new[field]

    for c in range(3, columns + 1):
        first(c)
    for c in range(4, columns):
        second(c)
    for side, (outer, steps, last) in enumerate(
        ((1, (1, 2), (2, 3)), (columns + 2, (columns + 2, columns + 1), (columns + 1, columns)))
    ):
        along[side].wait_recv()
        corners[side].wait_recv()
        for field in range(2):
            place(field, outer, relayed[side], (1 - side) * (columns - 1))
        for c in steps:
            first(c)
        for c in last:
            second(c)

    pairs = columns // 2
    for field in range(2):
        twos = [level[field][2 * k] + level[field][2 * k + 1] for k in range(pairs)]
        fours = [twos[2 * q] + twos[2 * q + 1] for q in range(pairs // 2)]
        for k in range(pairs):
            rows = pl.ds(field * planes * pairs + k, planes, stride=pairs)
            for tile in range(tiles):
                lanes = slice(tile * LANES, (tile + 1) * LANES)
                sums[tile, rows, :] = twos[k][:, lanes]
                sums[tiles + tile, rows, :] = fours[k // 2][:, lanes]

    contract = (((1,), (1,)), ((), ()))
    high, low = split(jnp.concatenate([sums[tile] for tile in range(2 * tiles)], axis=1))
    blend = lax.dot_general(to_blend, high, contract, preferred_element_type=jnp.float32)
    blend += lax.dot_general(to_blend, low, contract, preferred_element_type=jnp.float32)
    portion = half // owners
    for owner in range(owners):
        outgoing[owner] = blend[owner * portion : (owner + 1) * portion]

    deals = []
    for step in range(owners - 1, 0, -1):
        partner = partner_of(gy, step, owners)
        deals.append(
            pltpu.make_async_remote_copy(
                src_ref=outgoing.at[partner],
                dst_ref=gathered.at[gy],
                send_sem=deal_send.at[step - 1],
                recv_sem=deal_recv.at[step - 1],
                device_id=(gx, partner),
                device_id_type=MESH,
            )
        )
        deals[-1].start()
    gathered[gy] = outgoing[gy]

    for deal in deals:
        deal.wait_recv()

    for copy in across + along + corners:
        copy.wait_send()
    for deal in deals:
        deal.wait_send()


def finish(u_ref, v_ref, dealt, u_out, v_out, rebuilt_out, doubled, rebuilt, sems):
    copies = [
        pltpu.make_async_copy(u_ref, u_out, sems.at[0]),
        pltpu.make_async_copy(v_ref, v_out, sems.at[1]),
    ]
    for copy in copies:
        copy.start()

    owners, portion, _ = dealt.shape
    wide_in = lax.broadcasted_iota(jnp.int32, (LANES, 4 * LANES), 0)
    wide_out = lax.broadcasted_iota(jnp.int32, (LANES, 4 * LANES), 1)
    column_of = wide_in // 16 * 4 + wide_in % 4
    spreading = jnp.where(
        (wide_in // 4 % 4 == wide_out // LANES) & (column_of == wide_out % LANES // 2),
        1.0,
        0.0,
    ).astype(jnp.bfloat16)
    lane = lax.broadcasted_iota(jnp.int32, (portion, LANES), 1)
    blocks = [dealt[owner] for owner in range(owners)]
    width, rows = rebuilt.shape[1], 2 * portion
    chunks = 4
    share = 8 // chunks
    for chunk in range(chunks):
        for h in range(chunk * share, (chunk + 1) * share):
            part = jnp.zeros((portion, LANES), jnp.float32)
            for owner in range(8):
                shift = (16 * (owner - h)) % LANES
                moved = pltpu.roll(blocks[owner], shift, 1) if shift else blocks[owner]
                part = jnp.where(lane // 16 == owner, moved, part)
            doubled[pl.ds(h * rows, portion, stride=2), :] = part
            doubled[pl.ds(h * rows + 1, portion, stride=2), :] = part
        high, low = split(doubled[chunk * share * rows : (chunk + 1) * share * rows, :])
        whole = jnp.dot(high, spreading, preferred_element_type=jnp.float32)
        whole += jnp.dot(low, spreading, preferred_element_type=jnp.float32)
        for h in range(share):
            for z in range(4):
                base = ((chunk * share + h) * 4 + z) * rows
                rebuilt[base : base + rows, :] = whole[
                    h * rows : (h + 1) * rows, z * LANES : z * LANES + width
                ]
        size = share * 4 * rows
        copies.append(
            pltpu.make_async_copy(
                rebuilt.at[chunk * size : (chunk + 1) * size],
                rebuilt_out.at[chunk * size : (chunk + 1) * size],
                sems.at[2 + chunk],
            )
        )
        copies[-1].start()
    for copy in copies:
        copy.wait()


def tiled(field):
    planes, columns, extent = field.shape
    field = field.reshape(planes, columns, extent // LANES, LANES)
    return jnp.transpose(field, (0, 2, 1, 3)).reshape(-1, LANES)


def untiled(field, shape):
    planes, columns, extent = shape
    field = field.reshape(planes, extent // LANES, columns, LANES)
    return jnp.transpose(field, (0, 2, 1, 3)).reshape(shape)


def body(substrate, catalyst):
    planes, columns, extent = substrate.shape
    slabs_x, owners = lax.axis_size("gx"), lax.axis_size("gy")
    half, pairs, tiles = extent // 2, columns // 2, extent // LANES
    portion = half // owners
    values = 2 * planes * pairs
    fused = (
        planes == 16 and pairs == 4 and owners == 8 and values == LANES and portion % 8 == 0
    )
    dims = (planes, columns, extent, owners, slabs_x, owners)
    f32 = jnp.float32
    flat = (planes * tiles * columns, LANES)
    vmem = pl.BlockSpec(memory_space=pltpu.VMEM)
    anywhere = pl.BlockSpec(memory_space=pl.ANY)
    u, v, dealt = pl.pallas_call(
        functools.partial(kernel, dims),
        out_shape=(
            pltpu.VMEM(flat, f32),
            pltpu.VMEM(flat, f32),
            pltpu.VMEM((owners, portion, values), f32),
        ),
        in_specs=[anywhere] * 2,
        out_specs=(vmem,) * 3,
        scratch_shapes=[
            pltpu.VMEM((2,) + flat, f32),
            pltpu.VMEM((2, columns + 4, planes, extent), f32),
            pltpu.VMEM((2, columns + 4, planes, LANES), f32),
            pltpu.VMEM((planes, LANES), f32),
            pltpu.VMEM((2, planes, LANES), f32),
            pltpu.VMEM((planes, LANES), f32),
            pltpu.VMEM((2, planes, LANES), f32),
            pltpu.VMEM((2, columns + 4, planes, extent + LANES), f32),
            pltpu.VMEM((2 * tiles, values, LANES), f32),
            pltpu.VMEM((owners, portion, values), f32),
            pltpu.SemaphoreType.DMA((2,)),
            pltpu.SemaphoreType.DMA((6,)),
            pltpu.SemaphoreType.DMA((6,)),
            pltpu.SemaphoreType.DMA((owners - 1,)),
            pltpu.SemaphoreType.DMA((owners - 1,)),
        ],
        compiler_params=pltpu.CompilerParams(collective_id=0, has_side_effects=True),
    )(tiled(substrate), tiled(catalyst))
    rows, width = 2 * portion, columns * owners
    if fused:
        u, v, dealt = (
            pltpu.with_memory_space_constraint(x, pltpu.VMEM) for x in (u, v, dealt)
        )
        u, v, rebuilt = pl.pallas_call(
            finish,
            out_shape=(
                jax.ShapeDtypeStruct(flat, f32),
                jax.ShapeDtypeStruct(flat, f32),
                jax.ShapeDtypeStruct((2 * planes * rows, width), f32),
            ),
            in_specs=[vmem] * 3,
            out_specs=(anywhere,) * 3,
            scratch_shapes=[
                pltpu.VMEM((8 * rows, LANES), f32),
                pltpu.VMEM((2 * planes * rows, width), f32),
                pltpu.SemaphoreType.DMA((6,)),
            ],
        )(u, v, dealt)
        rebuilt = rebuilt.reshape(2, planes, rows, width)
    else:
        blend = dealt.reshape(owners, portion, 2, planes, pairs)
        blend = jnp.transpose(blend, (2, 3, 1, 0, 4)).reshape(2, planes, portion, owners * pairs)
        rebuilt = jnp.repeat(jnp.repeat(blend, 2, axis=2), 2, axis=3)
    return untiled(u, substrate.shape), untiled(v, substrate.shape), rebuilt


def solution(mesh):
    in_specs = (P(None, "gy", "gx"), P(None, "gy", "gx"))
    out_specs = (P(None, "gy", "gx"), P(None, "gy", "gx"), P(None, None, ("gx", "gy"), None))
    return jax.shard_map(body, mesh=mesh, in_specs=in_specs, out_specs=out_specs, check_vma=False)
```
